128 devices in a mesh: grp: 4 (over y, x), gx: 32 (over z, core).
Axes of the slice: x: 2, y: 2, z: 16, core: 2. Of those that a mesh axis runs over, the one named last changes fastest.
The devices are a block of a 8x8x16 slice.
Arguments:
- remaining_states: bfloat16 [512, 16384], P(('grp', 'gx')), parts along dimension 0, may hold values from -6 to 6
- scaling_factor_vector: bfloat16 [16384], replicated, may hold values from 0.25 to 1.75
- probe_projection_matrix: bfloat16 [16384, 8192], P(None, 'gx'), may hold values from -1 to 1
- memory_projection_matrix: bfloat16 [16384, 1024], P('gx'), may hold values from -0.046875 to 0.046875
- final_projection_matrix: bfloat16 [8192, 16384], P('gx'), may hold values from -0.0625 to 0.0625
- memorized_address_tensor: bfloat16 [4096, 128, 512], P(('grp', 'gx')), parts along dimension 0, may hold values from -8 to 8
- memorized_content_tensor: bfloat16 [4096, 128, 512], P(('grp', 'gx')), parts along dimension 0, may hold values from -6 to 6
- retained_sequence_ids: int32 [512], P('grp'), parts along dimension 0, may hold values from 0 to 1023, as said below
- occupied_positions: int32 [4096], P(('grp', 'gx')), parts along dimension 0, may hold values from 1 to 128
Outputs:
- result: bfloat16 [512, 16384], P(('grp', 'gx')), parts along dimension 0
The draws below stay inside these ranges and needn't reach their ends.
There are 4 independent parts, one for each index of `grp`. The reference program is written for one: setup_inputs(seed, part) draws one part's arguments, and reference() takes and returns one part's arrays. A program takes and returns all parts, laid end to end along the dimension named above; an argument that names none is the same for every part. Nothing has to cross between parts.
Inputs may be any that keep to these rules, and one draw needn't show every extreme that they name: Distinct batch rows; row r of remaining_states belongs to batch row retained_sequence_ids[r].
All inputs are finite; a program needn't handle non-finite values.
Results may differ from the reference program's by a relative error of at most 0.014.
Values may be sent and summed in bfloat16 or wider, within the bound.
A program may use at most 192 MiB of HBM per device.

```python
import math
import jax
import jax.numpy as jnp
from jax import lax

D = 16384
HEADS = 64
KV = 4
DH = 128
CACHE = 128
ROWS = 128
BATCH = 1024


def draw_remaining_states(key, part):
    sampled = jax.random.truncated_normal(key, -6.0, 6.0, (ROWS, D), jnp.float32)
    return sampled.astype(jnp.bfloat16)


def draw_probe_projection_matrix(key, part):
    scale = 1.0 / math.sqrt(D)
    columns_all = HEADS * DH
    sampled = jax.random.truncated_normal(key, -4.0, 4.0, (D, columns_all), jnp.float32) * scale
    return sampled.astype(jnp.bfloat16)


def draw_memorized_address_tensor(key, part):
    sampled = jax.random.truncated_normal(key, -6.0, 6.0, (BATCH, CACHE, KV * DH), jnp.float32)
    return sampled.astype(jnp.bfloat16)


def draw_retained_sequence_ids(key, part):
    shuffled = jax.random.permutation(key, BATCH)
    return shuffled[:ROWS].astype(jnp.int32)


def place_ends(values, rng, least, top_value):
    longest = values.shape.index(max(values.shape))
    spots = []
    for shift in (0, 1):
        where = [jax.random.randint(jax.random.fold_in(rng, axis), (), 0, length) for axis, length in enumerate(values.shape)]
        where[longest] = (where[longest] + shift) % values.shape[longest]
        spots.append(tuple(where))
    return values.at[spots[0]].set(least).at[spots[1]].set(top_value)


def shard_levels(rng, extent, split, low, top_value):
    def one(dim, parts):
        draws = jax.random.uniform(jax.random.fold_in(jax.random.fold_in(rng, 6), dim), (parts,), jnp.float32, low / len(split), top_value / len(split))
        return jnp.repeat(jnp.exp(draws), extent[dim] // parts).reshape((-1,) + (1,) * (len(extent) - dim - 1))

    loudness = one(*split[0])
    for cut in split[1:]:
        loudness = loudness * one(*cut)
    return loudness


def centred(own_key, extent, deviation, limit, split=(), held_as=jnp.bfloat16):
    drawn = jax.random.normal(own_key, extent, jnp.float32) * deviation
    if len(split) > 0:
        drawn = shard_levels(own_key, extent, split, -0.22, 0.18) * drawn
    return jnp.clip(drawn, min=-limit, max=limit).astype(held_as)


def setup_inputs(seed: int = 0, part: int = 0) -> dict:
    seeds = jax.random.split(jax.random.key(seed), 10)
    own_keys = jax.random.split(jax.random.fold_in(seeds[9], part), 10)
    remaining_states = draw_remaining_states(jax.random.fold_in(jax.random.fold_in(seeds[9], part), 71), part)
    scaling_factor_vector = jnp.clip(1.0 + 0.15 * jax.random.normal(seeds[1], (D,), jnp.float32), 0.25, 1.75).astype(jnp.bfloat16)
    probe_projection_matrix = draw_probe_projection_matrix(jax.random.fold_in(seeds[9], 71), part)
    memory_projection_matrix = centred(seeds[3], (D, 2 * KV * DH), D ** -0.5, 0.046875, ((0, 32),))
    final_projection_matrix = centred(seeds[4], (HEADS * DH, D), (HEADS * DH) ** -0.5, 0.0625, ((0, 32),))
    memorized_address_tensor = draw_memorized_address_tensor(jax.random.fold_in(jax.random.fold_in(seeds[9], part), 71), part)
    memorized_content_tensor = centred(own_keys[6], (BATCH, CACHE, KV * DH), 1.0, 6.0, ((0, 32),))
    retained_sequence_ids = draw_retained_sequence_ids(jax.random.fold_in(jax.random.fold_in(seeds[9], part), 71), part)
    occupied_positions = place_ends(jax.random.randint(own_keys[8], (BATCH,), 1, CACHE + 1), jax.random.fold_in(own_keys[8], 1), 1, CACHE).astype(jnp.int32)
    return dict(remaining_states=remaining_states, scaling_factor_vector=scaling_factor_vector, probe_projection_matrix=probe_projection_matrix, memory_projection_matrix=memory_projection_matrix, final_projection_matrix=final_projection_matrix, memorized_address_tensor=memorized_address_tensor, memorized_content_tensor=memorized_content_tensor, retained_sequence_ids=retained_sequence_ids, occupied_positions=occupied_positions)


epsilon = 1e-05

def attend_rows(probe_vectors, new_kv, keys, values, retained_fill_counts):
    slots = probe_vectors.shape[0]
    query_heads = probe_vectors.astype(jnp.float32).reshape(slots, KV, HEADS // KV, DH)
    key_heads = keys.astype(jnp.float32).reshape(slots, CACHE, KV, DH)
    value_heads = values.astype(jnp.float32).reshape(slots, CACHE, KV, DH)
    inverse = 1.0 / jnp.sqrt(jnp.float32(DH))
    scores = jnp.einsum('skgd,sjkd->skgj', query_heads, key_heads) * inverse
    visible = (jnp.arange(CACHE, dtype=jnp.int32)[None, :] < retained_fill_counts[:, None])[:, None, None, :]
    scores = jnp.where(visible, scores, jnp.float32(-1e+30))
    new_keys = new_kv[:, :KV * DH].astype(jnp.float32).reshape(slots, KV, 1, DH)
    new_values = new_kv[:, KV * DH:].astype(jnp.float32).reshape(slots, KV, 1, DH)
    own_score = lax.optimization_barrier(jnp.sum(query_heads * new_keys, axis=-1)) * inverse
    highest = jnp.maximum(lax.optimization_barrier(jnp.max(scores, axis=-1)), own_score)
    expo_cache = jnp.where(visible, jnp.exp(scores - highest[..., None]), jnp.float32(0.0))
    expo_new = jnp.exp(own_score - highest)
    denominator = lax.optimization_barrier(jnp.sum(expo_cache, axis=-1)) + expo_new
    weights = (expo_cache / denominator[..., None]).astype(jnp.bfloat16)
    weight_new = (expo_new / denominator).astype(jnp.bfloat16)
    summed = jnp.einsum('skgj,sjkd->skgd', weights.astype(jnp.float32), value_heads)
    summed = summed + weight_new.astype(jnp.float32)[..., None] * new_values
    return summed.reshape(slots, HEADS * DH).astype(jnp.bfloat16)

def reference(remaining_states, scaling_factor_vector, probe_projection_matrix, memory_projection_matrix, final_projection_matrix, memorized_address_tensor, memorized_content_tensor, retained_sequence_ids, occupied_positions):
    values = remaining_states.astype(jnp.float32)
    inverse = lax.rsqrt(lax.optimization_barrier(jnp.mean(values * values, axis=1, keepdims=True)) + epsilon)
    normed = (values * inverse * scaling_factor_vector.astype(jnp.float32)).astype(jnp.bfloat16)
    probe_vectors = jnp.dot(normed, probe_projection_matrix, preferred_element_type=jnp.float32).astype(jnp.bfloat16)
    new_kv = jnp.dot(normed, memory_projection_matrix, preferred_element_type=jnp.float32).astype(jnp.bfloat16)
    retained_address_tensor = memorized_address_tensor[retained_sequence_ids]
    retained_content_tensor = memorized_content_tensor[retained_sequence_ids]
    retained_fill_counts = occupied_positions[retained_sequence_ids]
    attended = attend_rows(probe_vectors, new_kv, retained_address_tensor, retained_content_tensor, retained_fill_counts)
    projected = jnp.dot(attended, final_projection_matrix, preferred_element_type=jnp.float32)
    return (values + projected).astype(jnp.bfloat16)
```

```python
import functools
import math

import jax
import jax.numpy as jnp
from jax import lax
from jax.experimental import pallas as pl
from jax.experimental.pallas import tpu as pltpu
from jax.sharding import PartitionSpec as P

HEADS = 64
KV = 4
DH = 128
EPS = 1e-05
MESH = pl.DeviceIdType.MESH
F32 = jnp.float32
BF16 = jnp.bfloat16


class Place:
    def __init__(self, n):
        self.n = n
        self.chips = n // 2
        self.me = lax.axis_index("gx")
        self.c = lax.rem(self.me, 2)
        self.z = lax.div(self.me, 2)
        self.up = lax.rem(self.me + 2, n)
        self.dn = lax.rem(self.me + n - 2, n)
        self.sib = self.me + 1 - 2 * self.c

    def chip(self, offset):
        return lax.rem(self.z + offset + 2 * self.chips, self.chips)

    def greet(self):
        barrier = pltpu.get_barrier_semaphore()
        for other in (self.up, self.dn, self.sib):
            pl.semaphore_signal(barrier, inc=1, device_id={"gx": other}, device_id_type=MESH)
        pl.semaphore_wait(barrier, 3)


def remote(src, dst, send_sem, recv_sem, device):
    return pltpu.make_async_remote_copy(
        src_ref=src,
        dst_ref=dst,
        send_sem=send_sem,
        recv_sem=recv_sem,
        device_id={"gx": device},
        device_id_type=MESH,
    )


def wait_bytes(ref, sem):
    pltpu.make_async_copy(ref, ref, sem).wait()


def gather_kernel(
    n,
    nj,
    nq,
    states,
    gain,
    wq_hbm,
    wkv_hbm,
    qall,
    kvall,
    xs,
    x32,
    nb,
    wq,
    wkv,
    acc,
    kvp,
    kvs,
    kvu,
    kvd,
    w_sem,
    x_sem,
    a_send,
    a_ru,
    a_rd,
    a_fs,
    a_fr,
    q_send,
    q_ru,
    q_rd,
    q_fs,
    q_fr,
    s_sem,
    r_send,
    r_ru,
    r_rd,
    g_send,
    g_ru,
    g_rd,
    g_fs,
    g_fr,
):
    p = Place(n)
    me, c, z = p.me, p.c, p.z
    chips = p.chips
    ups, dns = chips // 2, chips - 1 - chips // 2
    d = states.shape[1]
    kc = d // (2 * nj)

    wq_copy = pltpu.make_async_copy(wq_hbm, wq, w_sem.at[0])
    wkv_copy = pltpu.make_async_copy(wkv_hbm, wkv, w_sem.at[1])
    wq_copy.start()
    wkv_copy.start()

    p.greet()
    raw = remote(states, xs, x_sem.at[0], x_sem.at[1], p.sib)
    raw.start()
    raw.wait()

    first = c == 0
    total = jnp.zeros((8, 1), F32)
    for k in range(2 * nj):
        cols = pl.ds(k * kc, kc)
        own = states[:, cols].astype(F32)
        other = xs[:, cols].astype(F32)
        rows = jnp.concatenate(
            [jnp.where(first, own, other), jnp.where(first, other, own)], axis=0
        )
        x32[:, cols] = rows
        total = total + jnp.sum(rows * rows, axis=1, keepdims=True)
    inverse = lax.rsqrt(total / d + EPS)
    for k in range(2 * nj):
        cols = pl.ds(k * kc, kc)
        nb[k, z] = (x32[:, cols] * inverse * gain[:, cols].astype(F32)).astype(BF16)

    def a_part(j, origin):
        return nb.at[c * nj + j, origin]

    def a_up(t, j):
        ref = a_part(j, p.chip(1 - t))
        return remote(ref, ref, a_send.at[0, j], a_ru.at[t - 1, j], p.up)

    def a_dn(t, j):
        ref = a_part(j, p.chip(t - 1))
        return remote(ref, ref, a_send.at[1, j], a_rd.at[t - 1, j], p.dn)

    def a_forward(j, origin):
        ref = a_part(j, origin)
        remote(ref, ref, a_fs.at[j], a_fr.at[j], p.sib).start()

    def a_take_up(t, j):
        ref = a_part(j, p.chip(-t))
        remote(ref, ref, a_send.at[0, j], a_ru.at[t - 1, j], p.up).wait_recv()

    def a_take_dn(t, j):
        ref = a_part(j, p.chip(t))
        remote(ref, ref, a_send.at[1, j], a_rd.at[t - 1, j], p.dn).wait_recv()

    for j in range(nj):
        a_up(1, j).start()
        a_dn(1, j).start()

    def a_step(t, carry):
        for j in range(nj):
            a_take_up(t - 1, j)
            a_up(t, j).start()
            a_take_dn(t - 1, j)
            a_dn(t, j).start()
            a_forward(j, p.chip(1 - t))
            a_forward(j, p.chip(t - 1))
        return carry

    lax.fori_loop(2, dns + 1, a_step, 0)
    for j in range(nj):
        a_take_up(ups - 1, j)
        a_up(ups, j).start()
        a_take_dn(dns, j)
        a_forward(j, p.chip(1 - ups))
        a_forward(j, p.chip(dns))

    wq_copy.wait()
    wkv_copy.wait()

    def q_part(k):
        lhs = nb[k].reshape(8 * chips, kc)
        rhs = wq[pl.ds(pl.multiple_of(k * kc, kc), kc), :]
        return jnp.dot(lhs, rhs, preferred_element_type=F32)

    for j in range(nj):
        a_take_up(ups, j)
        a_forward(j, p.chip(-ups))
        part = q_part(c * nj + j)
        acc[...] = part if j == 0 else acc[...] + part
    for j in range(nj):
        k = (1 - c) * nj + j
        wait_bytes(nb.at[k, pl.ds(0, chips - 1)], a_fr.at[j])
        acc[...] += q_part(k)

    width = wkv.shape[0]
    per = kc // width
    k_own = lax.div(me, per)
    off = pl.multiple_of(lax.rem(me, per) * width, width)
    lhs = nb[k_own, :, :, pl.ds(off, width)].reshape(8 * chips, width)
    half = wkv.shape[1] // 2
    for h in range(2):
        kvp[h] = jnp.dot(
            lhs, wkv[:, h * half : (h + 1) * half], preferred_element_type=F32
        ).reshape(chips, 8, half)
    qall[me] = acc[...].astype(BF16)

    rows = 8 * chips // nq

    def q_block(j, origin):
        return qall.at[2 * origin + c, pl.ds(j * rows, rows)]

    def q_up(t, j):
        ref = q_block(j, p.chip(1 - t))
        return remote(ref, ref, q_send.at[0, j], q_ru.at[t - 1, j], p.up)

    def q_dn(t, j):
        ref = q_block(j, p.chip(t - 1))
        return remote(ref, ref, q_send.at[1, j], q_rd.at[t - 1, j], p.dn)

    def q_take_up(t, j):
        ref = q_block(j, p.chip(-t))
        remote(ref, ref, q_send.at[0, j], q_ru.at[t - 1, j], p.up).wait_recv()

    def q_take_dn(t, j):
        ref = q_block(j, p.chip(t))
        remote(ref, ref, q_send.at[1, j], q_rd.at[t - 1, j], p.dn).wait_recv()

    def q_forward(j, origin):
        ref = q_block(j, origin)
        remote(ref, ref, q_fs.at[j], q_fr.at[j], p.sib).start()

    for j in range(nq):
        q_up(1, j).start()
        q_dn(1, j).start()
    swap = remote(kvp.at[1 - c], kvs, s_sem.at[0], s_sem.at[1], p.sib)
    swap.start()
    for j in range(nq):
        q_forward(j, z)
    swap.wait_recv()

    def r_up(t):
        return remote(kvu.at[t - 1], kvu.at[t], r_send.at[0, t - 1], r_ru.at[t - 1], p.up)

    def r_dn(t):
        return remote(kvd.at[t - 1], kvd.at[t], r_send.at[1, t - 1], r_rd.at[t - 1], p.dn)

    def kv_own(chip):
        return kvp[c, chip] + kvs[chip]

    kvu[0] = kv_own(p.chip(ups))
    r_up(1).start()
    kvd[0] = kv_own(p.chip(-dns))
    r_dn(1).start()

    def r_up_step(t):
        r_up(t - 1).wait_recv()
        kvu[t - 1] += kv_own(p.chip(ups + 1 - t))
        r_up(t).start()

    def r_dn_step(t):
        r_dn(t - 1).wait_recv()
        kvd[t - 1] += kv_own(p.chip(t - 1 - dns))
        r_dn(t).start()

    def q_step(t, carry):
        for j in range(nq):
            q_take_up(t - 1, j)
            q_up(t, j).start()
            q_take_dn(t - 1, j)
            q_dn(t, j).start()
        r_up_step(t)
        r_dn_step(t)
        for j in range(nq):
            q_forward(j, p.chip(1 - t))
            q_forward(j, p.chip(t - 1))
        return carry

    lax.fori_loop(2, dns + 1, q_step, 0)
    for j in range(nq):
        q_take_up(ups - 1, j)
        q_up(ups, j).start()
        q_take_dn(dns, j)
    r_up_step(ups)
    for j in range(nq):
        q_forward(j, p.chip(1 - ups))
        q_forward(j, p.chip(dns))
    r_dn(dns).wait_recv()
    r_up(ups).wait_recv()
    kvall[c, z] = (kvu[ups] + kvd[dns] + kv_own(z)).astype(BF16)

    def g_part(origin):
        return kvall.at[c, origin]

    def g_up(t):
        ref = g_part(p.chip(1 - t))
        return remote(ref, ref, g_send.at[0], g_ru.at[t - 1], p.up)

    def g_dn(t):
        ref = g_part(p.chip(t - 1))
        return remote(ref, ref, g_send.at[1], g_rd.at[t - 1], p.dn)

    def g_take_up(t):
        ref = g_part(p.chip(-t))
        remote(ref, ref, g_send.at[0], g_ru.at[t - 1], p.up).wait_recv()

    def g_take_dn(t):
        ref = g_part(p.chip(t))
        remote(ref, ref, g_send.at[1], g_rd.at[t - 1], p.dn).wait_recv()

    def g_forward(origin):
        ref = g_part(origin)
        remote(ref, ref, g_fs.at[0], g_fr.at[0], p.sib).start()

    g_up(1).start()
    g_dn(1).start()
    g_forward(z)
    for j in range(nq):
        q_take_up(ups, j)
        q_forward(j, p.chip(-ups))

    def g_step(t, carry):
        g_take_up(t - 1)
        g_up(t).start()
        g_take_dn(t - 1)
        g_dn(t).start()
        g_forward(p.chip(1 - t))
        g_forward(p.chip(t - 1))
        return carry

    lax.fori_loop(2, dns + 1, g_step, 0)
    g_take_up(ups - 1)
    g_up(ups).start()
    g_take_dn(dns)
    g_forward(p.chip(1 - ups))
    g_forward(p.chip(dns))
    g_take_up(ups)
    g_forward(p.chip(-ups))

    for j in range(nj):
        wait_bytes(nb.at[0, pl.ds(0, ups)], a_send.at[0, j])
        wait_bytes(nb.at[0, pl.ds(0, dns)], a_send.at[1, j])
        wait_bytes(nb.at[0, pl.ds(0, chips - 1)], a_fs.at[j])
    for j in range(nq):
        wait_bytes(qall.at[pl.ds(0, ups), pl.ds(0, rows)], q_send.at[0, j])
        wait_bytes(qall.at[pl.ds(0, dns), pl.ds(0, rows)], q_send.at[1, j])
        wait_bytes(qall.at[pl.ds(0, chips), pl.ds(0, rows)], q_fs.at[j])
        wait_bytes(qall.at[pl.ds(0, chips), pl.ds(0, rows)], q_fr.at[j])
    swap.wait_send()

    def r_sent(t, carry):
        r_up(t).wait_send()
        r_dn(t).wait_send()
        return carry

    lax.fori_loop(1, dns + 1, r_sent, 0)
    r_up(ups).wait_send()
    wait_bytes(kvall.at[0, pl.ds(0, ups)], g_send.at[0])
    wait_bytes(kvall.at[0, pl.ds(0, dns)], g_send.at[1])
    wait_bytes(kvall.at[0], g_fs.at[0])
    wait_bytes(kvall.at[0], g_fr.at[0])


def gather(states, gain, wq, wkv, n):
    r, d = states.shape
    nj, nq = 4, 2
    chips = n // 2
    ups, dns = chips // 2, chips - 1 - chips // 2
    rows = 8 * chips
    width = wq.shape[1]
    half = wkv.shape[1] // 2
    dma = pltpu.SemaphoreType.DMA
    vmem = pltpu.VMEM
    return pl.pallas_call(
        functools.partial(gather_kernel, n, nj, nq),
        name="gather_queries",
        out_shape=(
            jax.ShapeDtypeStruct((n, rows, width), BF16),
            jax.ShapeDtypeStruct((2, chips, 8, half), BF16),
        ),
        in_specs=[pl.BlockSpec(memory_space=pltpu.VMEM)] * 2
        + [pl.BlockSpec(memory_space=pl.ANY)] * 2,
        out_specs=(pl.BlockSpec(memory_space=pltpu.VMEM),) * 2,
        scratch_shapes=[
            vmem((r, d), BF16),
            vmem((2 * r, d), F32),
            vmem((2 * nj, chips, 2 * r, d // (2 * nj)), BF16),
            vmem(wq.shape, BF16),
            vmem(wkv.shape, BF16),
            vmem((rows, width), F32),
            vmem((2, chips, 8, half), F32),
            vmem((chips, 8, half), F32),
            vmem((ups + 1, 8, half), F32),
            vmem((dns + 1, 8, half), F32),
            dma((2,)),
            dma((2,)),
            dma((2, nj)),
            dma((ups, nj)),
            dma((dns, nj)),
            dma((nj,)),
            dma((nj,)),
            dma((2, nq)),
            dma((ups, nq)),
            dma((dns, nq)),
            dma((nq,)),
            dma((nq,)),
            dma((2,)),
            dma((2, ups)),
            dma((ups,)),
            dma((dns,)),
            dma((2,)),
            dma((ups,)),
            dma((dns,)),
            dma((1,)),
            dma((1,)),
        ],
        compiler_params=pltpu.CompilerParams(collective_id=0, has_side_effects=True),
    )(states, gain, wq, wkv)


def attend_kernel(
    ids_s,
    occ_s,
    ids_row,
    ids_col,
    qall,
    kvall,
    k_hbm,
    v_hbm,
    out,
    slots_s,
    kbuf,
    vbuf,
    qs,
    att,
    new,
    k_sem,
    v_sem,
):
    slots, cache, _ = k_hbm.shape
    n, rows, width = qall.shape
    base = lax.axis_index("gx") * slots
    per = width // DH
    group = HEADS // KV

    def find(r, count):
        b = ids_s[r] - base
        mine = (b >= 0) & (b < slots)

        @pl.when(mine)
        def _():
            slots_s[count] = b
            pltpu.make_async_copy(k_hbm.at[b], kbuf.at[count], k_sem.at[count]).start()
            pltpu.make_async_copy(v_hbm.at[b], vbuf.at[count], v_sem.at[count]).start()

        return count + mine.astype(jnp.int32)

    count = lax.fori_loop(0, rows, find, jnp.int32(0))

    pick = (
        ids_row[...] - base == lax.broadcasted_iota(jnp.int32, (slots, rows), 0)
    ).astype(BF16)
    put = (
        ids_col[...] - base == lax.broadcasted_iota(jnp.int32, (rows, slots), 1)
    ).astype(BF16)
    for i in range(n):
        picked = jnp.dot(pick, qall[i], preferred_element_type=F32)
        for h in range(per):
            row = (i * per + h) * slots
            qs[row : row + slots, :] = picked[:, h * DH : (h + 1) * DH]
    for h in range(2):
        new[h] = jnp.dot(pick, kvall[h], preferred_element_type=F32)
    att[...] = jnp.zeros_like(att)

    scale = 1.0 / math.sqrt(DH)

    def one(i, carry):
        s = slots_s[i]
        filled = occ_s[s]
        pltpu.make_async_copy(k_hbm.at[0], kbuf.at[i], k_sem.at[i]).wait()
        pltpu.make_async_copy(v_hbm.at[0], vbuf.at[i], v_sem.at[i]).wait()
        q = qs[pl.ds(s, HEADS, stride=slots), :]
        q16 = q.astype(BF16)
        k_new = new[0, pl.ds(s, 1), :]
        v_new = new[1, pl.ds(s, 1), :]
        scores, own = [], []
        for g in range(KV):
            cols = slice(g * DH, (g + 1) * DH)
            head = slice(g * group, (g + 1) * group)
            scores.append(
                lax.dot_general(
                    q16[head],
                    kbuf[i, :, cols],
                    (((1,), (1,)), ((), ())),
                    preferred_element_type=F32,
                )
            )
            own.append(jnp.sum(q[head] * k_new[:, cols], axis=1, keepdims=True))
        scores = jnp.concatenate(scores, axis=0) * scale
        own = jnp.concatenate(own, axis=0) * scale
        visible = lax.broadcasted_iota(jnp.int32, (HEADS, cache), 1) < filled
        scores = jnp.where(visible, scores, -1e30)
        highest = jnp.maximum(jnp.max(scores, axis=1, keepdims=True), own)
        expo = jnp.where(visible, jnp.exp(scores - highest), 0.0)
        expo_new = jnp.exp(own - highest)
        denominator = jnp.sum(expo, axis=1, keepdims=True) + expo_new
        weights = (expo / denominator).astype(BF16)
        weight_new = (expo_new / denominator).astype(BF16).astype(F32)
        summed = []
        for g in range(KV):
            cols = slice(g * DH, (g + 1) * DH)
            head = slice(g * group, (g + 1) * group)
            part = jnp.dot(weights[head], vbuf[i, :, cols], preferred_element_type=F32)
            summed.append(part + weight_new[head] * v_new[:, cols])
        att[pl.ds(s, HEADS, stride=slots), :] = jnp.concatenate(summed, axis=0)
        return carry

    lax.fori_loop(0, count, one, 0)

    for i in range(n):
        block = jnp.concatenate(
            [
                att[(i * per + h) * slots : (i * per + h + 1) * slots, :].astype(BF16)
                for h in range(per)
            ],
            axis=1,
        )
        out[i] = jnp.dot(put, block, preferred_element_type=F32).astype(BF16)


def attend(ids, occ, qall, kvall, keys, values):
    n, rows, width = qall.shape
    slots, cache, lanes = keys.shape
    vm = pl.BlockSpec(memory_space=pltpu.VMEM)
    sm = pl.BlockSpec(memory_space=pltpu.SMEM)
    hbm = pl.BlockSpec(memory_space=pl.ANY)
    return pl.pallas_call(
        attend_kernel,
        name="attend_slots",
        out_shape=jax.ShapeDtypeStruct((n, rows, width), BF16),
        in_specs=[sm, sm, vm, vm, vm, vm, hbm, hbm],
        out_specs=vm,
        scratch_shapes=[
            pltpu.SMEM((slots + 1,), jnp.int32),
            pltpu.VMEM((slots, cache, lanes), BF16),
            pltpu.VMEM((slots, cache, lanes), BF16),
            pltpu.VMEM((HEADS * slots, DH), F32),
            pltpu.VMEM((HEADS * slots, DH), F32),
            pltpu.VMEM((2, slots, lanes), F32),
            pltpu.SemaphoreType.DMA((slots,)),
            pltpu.SemaphoreType.DMA((slots,)),
        ],
    )(ids, occ, ids.reshape(1, rows), ids.reshape(rows, 1), qall, kvall, keys, values)


def project_kernel(
    n,
    nd,
    nj,
    states,
    parts,
    wo_hbm,
    out,
    wo,
    sb,
    du,
    dd,
    mix,
    mine,
    theirs,
    heard,
    eu,
    ed,
    tail,
    tail_in,
    w_sem,
    b_send,
    b_recv,
    d_send,
    d_ru,
    d_rd,
    h_send,
    h_recv,
    e_send,
    e_ru,
    e_rd,
    t_send,
    t_recv,
):
    p = Place(n)
    c, z = p.c, p.z
    chips = p.chips
    ups, dns = chips // 2, chips - 1 - chips // 2
    d = states.shape[1]
    kc = d // (2 * nj)

    wo_copy = pltpu.make_async_copy(wo_hbm, wo, w_sem.at[0])
    wo_copy.start()
    p.greet()

    def b_copy(offset):
        chip = p.chip(offset)
        index = lax.rem(offset + chips, chips)
        return remote(
            parts.at[2 * chip + 1 - c], sb.at[chip], b_send.at[0], b_recv.at[index], p.sib
        )

    def b_take(offset):
        chip = p.chip(offset)
        index = lax.rem(offset + chips, chips)
        remote(
            parts.at[2 * chip + c], sb.at[chip], b_send.at[0], b_recv.at[index], p.sib
        ).wait_recv()

    def b_start(t, carry):
        b_copy(ups + 1 - t).start()
        b_copy(t - 1 - dns).start()
        return carry

    lax.fori_loop(1, dns + 1, b_start, 0)
    b_copy(jnp.int32(1)).start()
    b_copy(jnp.int32(0)).start()

    rows = 8 * chips // nd

    def d_up(t, j):
        part = pl.ds(j * rows, rows)
        return remote(
            du.at[t - 1, part], du.at[t, part], d_send.at[0, j], d_ru.at[t - 1, j], p.up
        )

    def d_dn(t, j):
        part = pl.ds(j * rows, rows)
        return remote(
            dd.at[t - 1, part], dd.at[t, part], d_send.at[1, j], d_rd.at[t - 1, j], p.dn
        )

    def d_own(chip, j):
        part = pl.ds(j * rows, rows)
        return parts[2 * chip + c, part, :] + sb[chip, part, :]

    b_take(jnp.int32(ups))
    for j in range(nd):
        du[0, pl.ds(j * rows, rows)] = d_own(p.chip(ups), j)
        d_up(1, j).start()
    b_take(jnp.int32(-dns))
    for j in range(nd):
        dd[0, pl.ds(j * rows, rows)] = d_own(p.chip(-dns), j)
        d_dn(1, j).start()

    def d_up_step(t):
        b_take(ups + 1 - t)
        for j in range(nd):
            d_up(t - 1, j).wait_recv()
            du[t - 1, pl.ds(j * rows, rows)] += d_own(p.chip(ups + 1 - t), j)
            d_up(t, j).start()

    def d_both_step(t, carry):
        b_take(ups + 1 - t)
        b_take(t - 1 - dns)
        for j in range(nd):
            part = pl.ds(j * rows, rows)
            d_up(t - 1, j).wait_recv()
            du[t - 1, part] += d_own(p.chip(ups + 1 - t), j)
            d_up(t, j).start()
            d_dn(t - 1, j).wait_recv()
            dd[t - 1, part] += d_own(p.chip(t - 1 - dns), j)
            d_dn(t, j).start()
        return carry

    lax.fori_loop(2, dns + 1, d_both_step, 0)
    d_up_step(jnp.int32(ups))
    b_take(jnp.int32(0))
    for j in range(nd):
        part = pl.ds(j * rows, rows)
        d_dn(dns, j).wait_recv()
        d_up(ups, j).wait_recv()
        mix[part] = du[ups, part] + dd[dns, part] + d_own(z, j)
    attended = mix[...]
    wo_copy.wait()

    def product(half, j):
        cols = pl.ds(pl.multiple_of(half * nj * kc + j * kc, kc), kc)
        value = jnp.dot(attended, wo[:, cols], preferred_element_type=F32)
        return value.reshape(chips, 8, kc)

    def h_copy(j):
        return remote(theirs.at[j], heard.at[j], h_send.at[j], h_recv.at[j], p.sib)

    def hand(j):
        theirs[j] = product(1 - c, j).astype(BF16)
        h_copy(j).start()

    def e_up(t, j):
        return remote(
            eu.at[t - 1, j], eu.at[t, j], e_send.at[0, j], e_ru.at[t - 1, j], p.up
        )

    def e_dn(t, j):
        return remote(
            ed.at[t - 1, j], ed.at[t, j], e_send.at[1, j], e_rd.at[t - 1, j], p.dn
        )

    def e_own(chip, j):
        return mine[j, chip] + heard[j, chip].astype(F32)

    hand(0)
    for j in range(nj):
        if j + 1 < nj:
            hand(j + 1)
        mine[j] = product(c, j)
        h_copy(j).wait_recv()
        eu[0, j] = e_own(p.chip(ups), j).astype(BF16)
        e_up(1, j).start()
        ed[0, j] = e_own(p.chip(-dns), j).astype(BF16)
        e_dn(1, j).start()

    def e_up_step(t, j):
        e_up(t - 1, j).wait_recv()
        eu[t - 1, j] = (eu[t - 1, j].astype(F32) + e_own(p.chip(ups + 1 - t), j)).astype(BF16)
        e_up(t, j).start()

    def e_dn_step(t, j):
        e_dn(t - 1, j).wait_recv()
        ed[t - 1, j] = (ed[t - 1, j].astype(F32) + e_own(p.chip(t - 1 - dns), j)).astype(BF16)
        e_dn(t, j).start()

    def e_step(t, carry):
        for j in range(nj):
            e_up_step(t, j)
            e_dn_step(t, j)
        return carry

    lax.fori_loop(2, dns + 1, e_step, 0)
    for j in range(nj):
        e_up_step(ups, j)

    first = c == 0

    def t_copy(j):
        return remote(tail.at[j], tail_in.at[j], t_send.at[j], t_recv.at[j], p.sib)

    def put(half, j, value):
        cols = pl.ds(pl.multiple_of(half * nj * kc + j * kc, kc), kc)
        out[:, cols] = (states[:, cols].astype(F32) + value).astype(BF16)

    for j in range(nj):
        e_dn(dns, j).wait_recv()
        e_up(ups, j).wait_recv()
        value = eu[ups, j].astype(F32) + ed[dns, j].astype(F32) + e_own(z, j)
        low, high = value[0:4], value[4:8]
        tail[j] = jnp.where(first, high, low)
        t_copy(j).start()
        put(c, j, jnp.where(first, low, high))
    for j in range(nj):
        t_copy(j).wait_recv()
        put(1 - c, j, tail_in[j])

    wait_bytes(sb, b_send.at[0])
    for j in range(nd):
        part = pl.ds(0, rows)
        wait_bytes(du.at[pl.ds(0, ups), part], d_send.at[0, j])
        wait_bytes(du.at[pl.ds(0, dns), part], d_send.at[1, j])
    for j in range(nj):
        h_copy(j).wait_send()
        wait_bytes(eu.at[pl.ds(0, ups), 0], e_send.at[0, j])
        wait_bytes(eu.at[pl.ds(0, dns), 0], e_send.at[1, j])
        t_copy(j).wait_send()


def project(states, parts, wo, n):
    r, d = states.shape
    nd, nj = 2, 4
    chips = n // 2
    ups, dns = chips // 2, chips - 1 - chips // 2
    rows = 8 * chips
    width = wo.shape[0]
    kc = d // (2 * nj)
    dma = pltpu.SemaphoreType.DMA
    vmem = pltpu.VMEM
    vm = pl.BlockSpec(memory_space=pltpu.VMEM)
    return pl.pallas_call(
        functools.partial(project_kernel, n, nd, nj),
        name="project_out",
        out_shape=jax.ShapeDtypeStruct((r, d), BF16),
        in_specs=[vm, vm, pl.BlockSpec(memory_space=pl.ANY)],
        out_specs=vm,
        scratch_shapes=[
            vmem(wo.shape, BF16),
            vmem((chips, rows, width), BF16),
            vmem((ups + 1, rows, width), BF16),
            vmem((dns + 1, rows, width), BF16),
            vmem((rows, width), BF16),
            vmem((nj, chips, 8, kc), F32),
            vmem((nj, chips, 8, kc), BF16),
            vmem((nj, chips, 8, kc), BF16),
            vmem((ups + 1, nj, 8, kc), BF16),
            vmem((dns + 1, nj, 8, kc), BF16),
            vmem((nj, 4, kc), F32),
            vmem((nj, 4, kc), F32),
            dma((1,)),
            dma((1,)),
            dma((chips,)),
            dma((2, nd)),
            dma((ups, nd)),
            dma((dns, nd)),
            dma((nj,)),
            dma((nj,)),
            dma((2, nj)),
            dma((ups, nj)),
            dma((dns, nj)),
            dma((nj,)),
            dma((nj,)),
        ],
        compiler_params=pltpu.CompilerParams(collective_id=1, has_side_effects=True),
    )(states, parts, wo)


def solution(mesh):
    n = mesh.shape["gx"]

    def local(states, gain, wq, wkv, wo, keys, values, ids, occ):
        qall, kvall = gather(states, gain.reshape(1, -1), wq, wkv, n)
        kvall = kvall.reshape(2, -1, kvall.shape[-1])
        parts = attend(ids, occ, qall, kvall, keys, values)
        return project(states, parts, wo, n)

    both = ("grp", "gx")
    placed = (
        P(both, None),
        P(),
        P(None, "gx"),
        P("gx", None),
        P("gx", None),
        P(both, None, None),
        P(both, None, None),
        P("grp"),
        P(both),
    )
    return jax.shard_map(
        local, mesh=mesh, in_specs=placed, out_specs=P(both, None), check_vma=False
    )
```
